256 devices in a mesh: section: 8 (over z), dp: 32 (over x, y, core).
Axes of the slice: x: 4, y: 4, z: 8, core: 2. Of those that a mesh axis runs over, the one named last changes fastest.
Arguments:
- inject: bfloat16 [8, 256, 4096], P('section', 'dp'), may hold values from -42 to 42, as said below
- w_gate: bfloat16 [8, 4096, 11008], P('section', None, 'dp'), may hold values from -0.09375 to 0.09375
- w_up: bfloat16 [8, 4096, 11008], P('section', None, 'dp'), may hold values from -0.09375 to 0.09375
- w_down: bfloat16 [8, 11008, 4096], P('section', 'dp'), may hold values from -0.0546875 to 0.0546875
- gain: float32 [8, 4096], P('section'), may hold values from 0.5 to 1.5
Outputs:
- iterate: float32 [8, 256, 4096], P('section', 'dp')
- mixing: float32 [8, 5, 5], P('section')
The draws below stay inside these ranges and needn't reach their ends.
Inputs may be any that keep to these rules, and one draw needn't show every extreme that they name: inject has entries of varied magnitude from token to token.
All inputs are finite; a program needn't handle non-finite values.
Results may differ from the reference program's by a relative error of at most 0.0038.
Values may be sent and summed in bfloat16 or wider, within the bound.
No kernel may reach another device: no remote copies, remote signals or barrier semaphores. Data moves between devices by JAX's collectives and lax.ppermute only.
A program may use at most 64 MiB of HBM per device.

```python
import math
import jax
import jax.numpy as jnp
from jax import lax

D = 4096
FF = 11008
ITERS = 5
HIST = 5
SECTIONS = 8
TOKENS = 256
N_DP = 32


def draw_inject(key, part):
    first = jax.random.fold_in(key, 11)
    second = jax.random.fold_in(key, 12)
    ramp = 3.0 ** (jnp.arange(TOKENS, dtype=jnp.float32) / TOKENS)
    base = jnp.clip(jax.random.normal(first, (SECTIONS, TOKENS, D), jnp.float32), -4.0, 4.0)
    scales = jnp.exp(jax.random.uniform(second, (SECTIONS, TOKENS, 1), jnp.float32, math.log(0.3), math.log(3.0)))
    values = jnp.clip(base * ramp[None, :, None] * scales, -42.0, 42.0)
    values = values.at[0, TOKENS - 1, 0].set(42.0).at[0, TOKENS - 1, 1].set(-42.0)
    return values.astype(jnp.bfloat16)


def block_levels(rng, dims, pieces, low, largest):
    def one(dim, parts):
        steps = jax.random.uniform(jax.random.fold_in(jax.random.fold_in(rng, 6), dim), (parts,), jnp.float32, low / len(pieces), largest / len(pieces))
        return jnp.repeat(jnp.exp(steps), dims[dim] // parts).reshape((-1,) + (1,) * (len(dims) - dim - 1))

    factor_of = one(*pieces[0])
    for cut in pieces[1:]:
        factor_of = factor_of * one(*cut)
    return factor_of


def bell_draw(rng, shape, spread, limit, shards=(), kind=jnp.bfloat16):
    factor_of = block_levels(rng, shape, shards, -0.22, 0.18) if shards else 1.0
    values = jax.random.normal(rng, shape, jnp.float32) * spread * factor_of
    return jnp.minimum(jnp.maximum(values, -limit), limit).astype(kind)


def setup_inputs(seed: int = 0) -> dict:
    splits = jax.random.split(jax.random.key(seed), 6)
    return {
        "inject": draw_inject(jax.random.fold_in(splits[5], 71), 0),
        "w_gate": bell_draw(splits[1], (SECTIONS, D, FF), D ** -0.5, 0.09375, ((0, 8), (2, 32))),
        "w_up": bell_draw(splits[2], (SECTIONS, D, FF), D ** -0.5, 0.09375, ((0, 8), (2, 32))),
        "w_down": bell_draw(splits[3], (SECTIONS, FF, D), FF ** -0.5, 0.0546875, ((0, 8), (1, 32))),
        "gain": jnp.clip(1.0 + 0.1 * jax.random.normal(splits[4], (SECTIONS, D), jnp.float32), 0.5, 1.5),
    }


def rms_scaled(values, gain_row):
    inverse = lax.rsqrt(lax.optimization_barrier(jnp.mean(values * values, axis=-1, keepdims=True)) + 1e-06)
    return (values * inverse * gain_row).astype(jnp.bfloat16)

def solve_small(system, target):
    count = system.shape[-1]
    entries = [[system[..., i, j] for j in range(count)] for i in range(count)]
    values = [target[..., i] for i in range(count)]
    for p in range(count):
        for i in range(p + 1, count):
            factor = entries[i][p] / entries[p][p]
            for j in range(p, count):
                entries[i][j] = entries[i][j] - factor * entries[p][j]
            values[i] = values[i] - factor * values[p]
    answer = [None] * count
    for i in range(count - 1, -1, -1):
        accum = values[i]
        for j in range(i + 1, count):
            accum = accum - entries[i][j] * answer[j]
        answer[i] = accum / entries[i][i]
    return jnp.stack(answer, axis=-1)

def mixing_weights(matrix, iteration):
    live = (jnp.arange(HIST) <= iteration).astype(jnp.float32)
    damp = 0.01 * jnp.trace(matrix, axis1=-2, axis2=-1) / (iteration + 1) + 1e-06
    eye_mat = jnp.eye(HIST, dtype=jnp.float32)
    diagonal = live * damp[..., None] + (1.0 - live)
    system = matrix * live[:, None] * live[None, :] + eye_mat * diagonal[..., None, :]
    target = jnp.broadcast_to(live, system.shape[:-1])
    beta = solve_small(system, target)
    return beta / lax.optimization_barrier(jnp.sum(beta, axis=-1, keepdims=True))

def block_out(operands):
    values, gate_w, up_w, down_w, gain_row = operands
    normed = rms_scaled(values, gain_row)
    gate_val = jnp.dot(normed, gate_w, preferred_element_type=jnp.float32)
    up_val = jnp.dot(normed, up_w, preferred_element_type=jnp.float32)
    hidden = (jax.nn.silu(gate_val) * up_val).astype(jnp.bfloat16)
    grouped = hidden.reshape(TOKENS, N_DP, FF // N_DP).transpose(1, 0, 2).astype(jnp.float32)
    down_groups = down_w.reshape(N_DP, FF // N_DP, D).astype(jnp.float32)
    partials = jnp.einsum('gtf,gfd->gtd', grouped, down_groups).astype(jnp.bfloat16).astype(jnp.float32)
    total = lax.optimization_barrier(jnp.sum(partials, axis=0))
    return (values + total).astype(jnp.bfloat16)

def reference(inject, w_gate, w_up, w_down, gain):
    source = inject.astype(jnp.float32)
    iterate = jnp.zeros((SECTIONS, TOKENS, D), jnp.float32)
    images = jnp.zeros((HIST, SECTIONS, TOKENS, D), jnp.float32)
    misfits = jnp.zeros((HIST, SECTIONS, TOKENS, D), jnp.float32)
    mixing = jnp.zeros((SECTIONS, ITERS, HIST), jnp.float32)
    cell_count = float(TOKENS * D)
    for iteration in range(ITERS):
        output = lax.map(block_out, (iterate, w_gate, w_up, w_down, gain))
        mapped = source + 0.5 * jnp.roll(output, 1, axis=0).astype(jnp.float32)
        misfit = mapped - iterate
        images = images.at[iteration].set(mapped)
        misfits = misfits.at[iteration].set(misfit)
        gram_matrix = jnp.einsum('hstd,gstd->shg', misfits, misfits, precision=lax.Precision.HIGHEST) / cell_count
        weights = mixing_weights(gram_matrix, iteration)
        mixing = mixing.at[:, iteration].set(weights)
        iterate = jnp.einsum('sh,hstd->std', weights, images, precision=lax.Precision.HIGHEST)
    return (iterate, mixing)
```

```python
import functools

import jax
import jax.numpy as jnp
from jax import lax
from jax.experimental import pallas as pl
from jax.experimental.pallas import tpu as pltpu
from jax.sharding import PartitionSpec as P

ITERS = 5
HIST = 5
F32 = jnp.float32
BF16 = jnp.bfloat16
EXTRA = 256


MIB = 1024 * 1024
RING = tuple(
    4 * x + y
    for x, y in ((0, 0), (0, 1), (0, 2), (0, 3), (1, 3), (1, 2), (1, 1), (2, 1))
    + ((2, 2), (2, 3), (3, 3), (3, 2), (3, 1), (3, 0), (2, 0), (1, 0))
)


def pallas(body, out_shape, name, limit, scratch=()):
    return pl.pallas_call(
        body,
        out_shape=out_shape,
        scratch_shapes=list(scratch),
        name=name,
        compiler_params=pltpu.CompilerParams(vmem_limit_bytes=limit * MIB),
    )


def silu_times(gate, up):
    return gate / (1.0 + jnp.exp(-gate)) * up


def normalized(values, gain):
    mean = jnp.mean(values * values, axis=-1, keepdims=True)
    return (values * lax.rsqrt(mean + 1e-06) * gain).astype(BF16)


def by_rows(a, b):
    return lax.dot_general(a, b, (((1,), (1,)), ((), ())), preferred_element_type=F32)


def start_body(gain_ref, gate_ref, up_ref, down_ref, part_ref):
    features = gate_ref.shape[1]
    normed = normalized(jnp.zeros((8, features), F32), gain_ref[...])
    gate = by_rows(normed, gate_ref[...])
    up = by_rows(normed, up_ref[...])
    act = silu_times(gate, up).astype(BF16)
    piece = features // 8
    row = lax.broadcasted_iota(jnp.int32, (8, piece), 0)
    folded = jnp.zeros((8, piece), F32)
    for r in range(8):
        out = jnp.dot(act, down_ref[:, r * piece : (r + 1) * piece], preferred_element_type=F32)
        folded = folded + jnp.where(row == r, out, 0.0)
    part_ref[...] = folded.astype(BF16)


def entry(row, lane):
    return row[:, lane : lane + 1]


def solved_weights(entries, iteration):
    count = iteration + 1
    trace = entries[0][0]
    for i in range(1, count):
        trace = trace + entries[i][i]
    damp = 0.01 * trace / count + 1e-06
    rows = [[entries[i][j] for j in range(count)] for i in range(count)]
    for i in range(count):
        rows[i][i] = rows[i][i] + damp
    values = [jnp.ones((1, 1), F32) for _ in range(count)]
    for p in range(count):
        for i in range(p + 1, count):
            factor = rows[i][p] / rows[p][p]
            for j in range(p, count):
                rows[i][j] = rows[i][j] - factor * rows[p][j]
            values[i] = values[i] - factor * values[p]
    beta = [None] * count
    for i in range(count - 1, -1, -1):
        accum = values[i]
        for j in range(i + 1, count):
            accum = accum - rows[i][j] * beta[j]
        beta[i] = accum / rows[i][i]
    total = beta[0]
    for i in range(1, count):
        total = total + beta[i]
    return [b / total for b in beta]


def lane_row(values):
    lane = lax.broadcasted_iota(jnp.int32, (1, 128), 1)
    out = jnp.zeros((1, 128), F32)
    for j, value in enumerate(values):
        out = out + jnp.where(lane == j, value, 0.0)
    return out


def gram_and_weights(extras, state, iteration, cells):
    chips = extras.shape[0] // 8
    sums = extras[0:8].astype(F32)
    for h in range(1, chips):
        sums = sums + extras[8 * h : 8 * h + 8].astype(F32)
    sums = sums[:, :128] + sums[:, 128:]
    fresh = (sums[2:3] + sums[1:2] + sums[0:1]) / cells
    known = [fresh] if state is None else [state[i : i + 1] for i in range(iteration)] + [fresh]
    if state is None:
        known = [lane_row([entry(fresh, 8)]), fresh]
    entries = [[None] * (iteration + 1) for _ in range(iteration + 1)]
    for i in range(iteration + 1):
        for j in range(i + 1):
            entries[i][j] = entries[j][i] = entry(known[i], j)
    weights = solved_weights(entries, iteration)
    kept = known + [jnp.zeros((8 - len(known), 128), F32)]
    return jnp.concatenate(kept, axis=0), weights, entries


def weight_rows(weights, entries, first):
    rows = [lane_row(weights)]
    if first:
        rows.append(lane_row(solved_weights(entries, 0)))
    rows.append(jnp.zeros((8 - len(rows), 128), F32))
    return jnp.concatenate(rows, axis=0)


def start_row(first_ref, features):
    tokens = first_ref.shape[0]
    sums = first_ref[0:8, features:].astype(F32)
    for h in range(1, tokens // 8):
        sums = sums + first_ref[8 * h : 8 * h + 8, features:].astype(F32)
    sums = sums.astype(BF16).astype(F32)
    return jnp.concatenate([sums[r : r + 1] for r in range(8)], axis=1)


def send_block(normed_ref, weights, part_ref):
    acts = []
    for gate_ref, up_ref in (weights[0:2], weights[3:5]):
        gate = by_rows(gate_ref[...], normed_ref[...])
        up = by_rows(up_ref[...], normed_ref[...])
        acts.append(jnp.transpose(silu_times(gate, up)).astype(BF16))
    features = part_ref.shape[1]
    step = min(512, features)
    for n in range(0, features, step):
        cols = slice(n, n + step)
        part = jnp.dot(acts[0], weights[2][:, cols], preferred_element_type=F32)
        part = part + jnp.dot(acts[1], weights[5][:, cols], preferred_element_type=F32)
        part_ref[:, cols] = part.astype(BF16)


def first_block_body(first_ref, own_ref, gain_ref, *refs):
    weights, (part_ref, image_ref, normed_ref) = refs[:6], refs[6:]
    tokens, features = part_ref.shape
    half = 0.5 * start_row(first_ref, features)
    image_ref[...] = own_ref[...].astype(F32) + half
    for h in range(0, tokens, 16):
        rows = first_ref[h : h + 16, :features].astype(F32) + half
        normed_ref[h : h + 16, :] = normalized(rows, gain_ref[...])
    send_block(normed_ref, weights, part_ref)


def block_body(iteration, cells, *refs):
    live = iteration
    first_ref = refs[0]
    outs = refs[1:live]
    images = refs[live : 2 * live]
    at = 2 * live
    state_ref = None
    if iteration > 2:
        state_ref = refs[at]
        at += 1
    gain_ref = refs[at]
    weights = refs[at + 1 : at + 7]
    part_ref, x_ref, kept_ref, mix_ref, normed_ref = refs[at + 7 :]
    tokens, features = part_ref.shape
    state = None if state_ref is None else state_ref[...]
    kept, mix, entries = gram_and_weights(outs[-1][:, features:], state, iteration - 1, cells)
    kept_ref[...] = kept
    mix_ref[...] = weight_rows(mix, entries, iteration == 2)
    x = mix[0] * images[0][...]
    for i in range(1, live):
        x = x + mix[i] * images[i][...]
    x_ref[...] = x
    total = mix[0]
    for i in range(1, live):
        total = total + mix[i]
    base = (0.5 * mix[0]) * start_row(first_ref, features)
    for h in range(0, tokens, 16):
        rows = total * first_ref[h : h + 16, :features].astype(F32) + base
        for i in range(1, live):
            rows = rows + (0.5 * mix[i]) * outs[i - 1][h : h + 16, :features].astype(F32)
        normed_ref[h : h + 16, :] = normalized(rows, gain_ref[...])
    send_block(normed_ref, weights, part_ref)


def split_in_three(values):
    high = values.astype(BF16).astype(F32)
    rest = values - high
    mid = rest.astype(BF16).astype(F32)
    low = rest - mid
    return [high, mid, low]


def inner(a, b):
    return jnp.sum(jnp.sum(a * b, axis=0, keepdims=True), axis=1, keepdims=True)


def image_body(iteration, before_ref, inject_ref, x_ref, *refs):
    misfits = refs[:iteration]
    image_ref, misfit_ref, extra_ref = refs[iteration:]
    image = inject_ref[...].astype(F32) + 0.5 * before_ref[...].astype(F32)
    misfit = image - x_ref[...]
    image_ref[...] = image
    misfit_ref[...] = misfit
    values = [inner(misfit, misfits[j][...]) for j in range(iteration)] + [inner(misfit, misfit)]
    row = lane_row(values)
    if iteration == 1:
        lane = lax.broadcasted_iota(jnp.int32, (1, 128), 1)
        first = misfits[0][...]
        row = row + jnp.where(lane == 8, inner(first, first), 0.0)
    pieces = split_in_three(row)
    extra_ref[...] = jnp.concatenate(pieces + [jnp.zeros((5, 128), F32)], axis=0).astype(BF16)


def final_body(cells, *refs):
    extra_ref = refs[0]
    images = refs[1 : 1 + HIST]
    state_ref = refs[1 + HIST]
    x_ref, mix_ref = refs[2 + HIST :]
    _, mix, entries = gram_and_weights(extra_ref[...], state_ref[...], ITERS - 1, cells)
    mix_ref[...] = weight_rows(mix, entries, False)
    x = mix[0] * images[0][...]
    for i in range(1, HIST):
        x = x + mix[i] * images[i][...]
    x_ref[...] = x


def local(inject, w_gate, w_up, w_down, gain):
    rows, features = inject.shape[1:]
    sections = lax.axis_size("section")
    groups = lax.axis_size("dp")
    chips = groups // 2
    tokens = rows * chips
    cells = float(rows * groups * features)
    hidden = w_gate.shape[2]
    order = RING if chips == len(RING) else tuple(range(chips))
    same_core = [[2 * h + c for h in order] for c in range(2)]
    across = [(d, d ^ 1) for d in range(groups)]
    ahead = [(s, (s + 1) % sections) for s in range(sections)]
    ahead_across = [
        (s * groups + d, (s + 1) % sections * groups + (d ^ 1))
        for s in range(sections)
        for d in range(groups)
    ]
    both = ("section", "dp")

    def to_chips(array):
        return lax.all_to_all(array, "dp", 0, 0, tiled=True, axis_index_groups=same_core)

    def to_all(block):
        wider = jnp.broadcast_to(block[None], (chips, *block.shape))
        return to_chips(wider).reshape(chips * block.shape[0], block.shape[1])

    shape = jax.ShapeDtypeStruct
    mine = inject[0]
    mine_w = [w_gate[0].T, w_up[0].T, w_down[0]]
    other_w = [lax.ppermute(w, "dp", across) for w in mine_w]
    part0 = pallas(start_body, shape((8, features // 8), BF16), "start", 12)(gain, *mine_w)
    near = lax.ppermute(part0, "section", ahead)
    far = lax.ppermute(part0, both, ahead_across)
    start_part = (near.astype(F32) + far.astype(F32)).astype(BF16)
    first = to_all(jnp.concatenate([mine, start_part], axis=1))

    part_shape = shape((tokens, features), BF16)
    own_shape = shape((rows, features), F32)
    small = shape((8, 128), F32)
    scratch = [pltpu.VMEM((tokens, features), BF16)]
    weights = mine_w + other_w
    images, misfits, gathered, mixing = [], [], [], []
    state = None
    for iteration in range(1, ITERS):
        if iteration == 1:
            part, x = pallas(first_block_body, (part_shape, own_shape), "block1", 12, scratch)(
                first, mine, gain, *weights
            )
            images.append(x)
            misfits.append(x)
        else:
            body = functools.partial(block_body, iteration, cells)
            carried = [] if state is None else [state]
            arrays = (first, *gathered, *images, *carried, gain, *weights)
            part, x, state, mix = pallas(
                body, (part_shape, own_shape, small, small), f"block{iteration}", 12, scratch
            )(first, *gathered, *images, *carried, gain, *weights)
            if iteration == 2:
                mixing.append(mix[1, :HIST])
            mixing.append(mix[0, :HIST])
        summed = jnp.sum(to_chips(part.reshape(chips, rows, features)).astype(F32), axis=0)
        before = lax.ppermute((x + summed).astype(BF16), "section", ahead)
        image, misfit, extra = pallas(
            functools.partial(image_body, iteration),
            (own_shape, own_shape, shape((8, 128), BF16)),
            f"image{iteration}",
            8,
        )(before, mine, x, *misfits)
        images.append(image)
        misfits.append(misfit)
        payload = [extra, lax.ppermute(extra, "dp", across)]
        if iteration < ITERS - 1:
            payload = [before] + payload
        gathered.append(to_all(jnp.concatenate(payload, axis=1)))
    iterate, mix = pallas(
        functools.partial(final_body, cells), (shape((rows, features), F32), small), "final", 8
    )(gathered[-1], *images, state)
    mixing.append(mix[0, :HIST])
    return iterate[None], jnp.stack(mixing)[None]


def solution(mesh):
    placed = (
        P("section", "dp", None),
        P("section", None, "dp"),
        P("section", None, "dp"),
        P("section", "dp", None),
        P("section", None),
    )
    return jax.shard_map(
        local,
        mesh=mesh,
        in_specs=placed,
        out_specs=(P("section", "dp", None), P("section", None, None)),
        check_vma=False,
    )
```

```python
import functools

import jax
import jax.numpy as jnp
from jax import lax
from jax.experimental import pallas as pl
from jax.experimental.pallas import tpu as pltpu
from jax.sharding import PartitionSpec as P

ITERS = 5
HIST = 5
F32 = jnp.float32
BF16 = jnp.bfloat16


MIB = 1024 * 1024
RING = tuple(
    4 * x + y
    for x, y in ((0, 0), (0, 1), (0, 2), (0, 3), (1, 3), (1, 2), (1, 1), (2, 1))
    + ((2, 2), (2, 3), (3, 3), (3, 2), (3, 1), (3, 0), (2, 0), (1, 0))
)


def pallas(body, out_shape, name, limit, scratch=(), places=None):
    options = {} if places is None else {"in_specs": places}
    return pl.pallas_call(
        body,
        out_shape=out_shape,
        scratch_shapes=list(scratch),
        name=name,
        compiler_params=pltpu.CompilerParams(vmem_limit_bytes=limit * MIB),
        **options,
    )


def silu_times(gate, up):
    return gate / (1.0 + jnp.exp(-gate)) * up


def normalized(values, gain):
    mean = jnp.mean(values * values, axis=-1, keepdims=True)
    return (values * lax.rsqrt(mean + 1e-06) * gain).astype(BF16)


def by_rows(a, b):
    return lax.dot_general(a, b, (((1,), (1,)), ((), ())), preferred_element_type=F32)


def start_body(gain_ref, *refs):
    sources, (part_ref, gate_ref, up_ref, down_ref, sems) = refs[:3], refs[3:]
    held = (gate_ref, up_ref, down_ref)
    copies = [pltpu.make_async_copy(sources[i], held[i], sems.at[i]) for i in range(3)]
    for copy in copies:
        copy.start()
    features = gate_ref.shape[1]
    normed = normalized(jnp.zeros((8, features), F32), gain_ref[...])
    copies[0].wait()
    gate = by_rows(normed, gate_ref[...])
    copies[1].wait()
    up = by_rows(normed, up_ref[...])
    act = silu_times(gate, up).astype(BF16)
    copies[2].wait()
    piece = features // 8
    row = lax.broadcasted_iota(jnp.int32, (8, piece), 0)
    folded = jnp.zeros((8, piece), F32)
    for r in range(8):
        out = jnp.dot(act, down_ref[:, r * piece : (r + 1) * piece], preferred_element_type=F32)
        folded = folded + jnp.where(row == r, out, 0.0)
    part_ref[...] = folded.astype(BF16)


def entry(row, lane):
    return row[:, lane : lane + 1]


def solved_weights(entries, iteration):
    count = iteration + 1
    trace = entries[0][0]
    for i in range(1, count):
        trace = trace + entries[i][i]
    damp = 0.01 * trace / count + 1e-06
    rows = [[entries[i][j] for j in range(count)] for i in range(count)]
    for i in range(count):
        rows[i][i] = rows[i][i] + damp
    values = [jnp.ones((1, 1), F32) for _ in range(count)]
    for p in range(count):
        for i in range(p + 1, count):
            factor = rows[i][p] / rows[p][p]
            for j in range(p, count):
                rows[i][j] = rows[i][j] - factor * rows[p][j]
            values[i] = values[i] - factor * values[p]
    beta = [None] * count
    for i in range(count - 1, -1, -1):
        accum = values[i]
        for j in range(i + 1, count):
            accum = accum - rows[i][j] * beta[j]
        beta[i] = accum / rows[i][i]
    total = beta[0]
    for i in range(1, count):
        total = total + beta[i]
    return [b / total for b in beta]


def lane_row(values):
    lane = lax.broadcasted_iota(jnp.int32, (1, 128), 1)
    out = jnp.zeros((1, 128), F32)
    for j, value in enumerate(values):
        out = out + jnp.where(lane == j, value, 0.0)
    return out


def gram_and_weights(fresh, state, iteration, cells):
    fresh = fresh[0:1] / cells
    if state is None:
        known = [lane_row([entry(fresh, 8)]), fresh]
    else:
        known = [state[i : i + 1] for i in range(iteration)] + [fresh]
    entries = [[None] * (iteration + 1) for _ in range(iteration + 1)]
    for i in range(iteration + 1):
        for j in range(i + 1):
            entries[i][j] = entries[j][i] = entry(known[i], j)
    weights = solved_weights(entries, iteration)
    kept = known + [jnp.zeros((8 - len(known), 128), F32)]
    return jnp.concatenate(kept, axis=0), weights, entries


def weight_rows(weights, entries, first):
    rows = [lane_row(weights)]
    if first:
        rows.append(lane_row(solved_weights(entries, 0)))
    rows.append(jnp.zeros((8 - len(rows), 128), F32))
    return jnp.concatenate(rows, axis=0)


def start_row(first_ref, features):
    tokens = first_ref.shape[0]
    sums = first_ref[0:8, features:].astype(F32)
    for h in range(1, tokens // 8):
        sums = sums + first_ref[8 * h : 8 * h + 8, features:].astype(F32)
    sums = sums.astype(BF16).astype(F32)
    return jnp.concatenate([sums[r : r + 1] for r in range(8)], axis=1)


def send_block(normed_ref, weights, part_ref):
    acts = []
    for gate_ref, up_ref in (weights[0:2], weights[3:5]):
        gate = by_rows(gate_ref[...], normed_ref[...])
        up = by_rows(up_ref[...], normed_ref[...])
        acts.append(jnp.transpose(silu_times(gate, up)).astype(BF16))
    features = part_ref.shape[1]
    step = min(512, features)
    for n in range(0, features, step):
        cols = slice(n, n + step)
        part = jnp.dot(acts[0], weights[2][:, cols], preferred_element_type=F32)
        part = part + jnp.dot(acts[1], weights[5][:, cols], preferred_element_type=F32)
        part_ref[:, cols] = part.astype(BF16)


def own_rows(x_ref, order):
    chip = lax.axis_index("dp") // 2
    slot = jnp.int32(0)
    for i, h in enumerate(order):
        slot = jnp.where(chip == h, i, slot)
    return x_ref[pl.ds(pl.multiple_of(8 * slot, 8), 8), :]


def first_block_body(order, first_ref, gain_ref, *refs):
    weights, (part_ref, x_ref, own_x_ref, normed_ref) = refs[:6], refs[6:]
    tokens, features = part_ref.shape
    half = 0.5 * start_row(first_ref, features)
    for h in range(0, tokens, 16):
        rows = first_ref[h : h + 16, :features].astype(F32) + half
        x_ref[h : h + 16, :] = rows
        normed_ref[h : h + 16, :] = normalized(rows, gain_ref[...])
    own_x_ref[...] = own_rows(x_ref, order)
    send_block(normed_ref, weights, part_ref)


def block_body(iteration, cells, order, *refs):
    own_ref, other_ref, first_ref = refs[:3]
    outs = refs[3 : 2 + iteration]
    at = 2 + iteration
    state = None
    if iteration > 2:
        state = refs[at][...]
        at += 1
    gain_ref = refs[at]
    weights = refs[at + 1 : at + 7]
    if iteration < ITERS - 1:
        part_ref, own_x_ref, kept_ref, mix_ref, x_ref, normed_ref = refs[at + 7 :]
    else:
        part_ref, own_x_ref, kept_ref, mix_ref, normed_ref, x_ref = refs[at + 7 :]
    tokens, features = part_ref.shape
    fresh = own_ref[...] + other_ref[...]
    kept, mix, entries = gram_and_weights(fresh, state, iteration - 1, cells)
    kept_ref[...] = kept
    mix_ref[...] = weight_rows(mix, entries, iteration == 2)
    total = mix[0]
    for i in range(1, iteration):
        total = total + mix[i]
    base = (0.5 * mix[0]) * start_row(first_ref, features)
    for h in range(0, tokens, 16):
        rows = total * first_ref[h : h + 16, :features].astype(F32) + base
        for i in range(1, iteration):
            rows = rows + (0.5 * mix[i]) * outs[i - 1][h : h + 16, :].astype(F32)
        x_ref[h : h + 16, :] = rows
        normed_ref[h : h + 16, :] = normalized(rows, gain_ref[...])
    own_x_ref[...] = own_rows(x_ref, order)
    send_block(normed_ref, weights, part_ref)


def folded_lanes(values):
    pieces = [values[:, n : n + 128] for n in range(0, values.shape[1], 128)]
    while len(pieces) > 1:
        pieces = [a + b for a, b in zip(pieces[::2], pieces[1::2])]
    return pieces[0]


def summed(values):
    return jnp.sum(jnp.sum(values, axis=0, keepdims=True), axis=1, keepdims=True)


def gram_row(sums, first):
    row = lane_row([summed(s) for s in sums])
    if first is not None:
        lane = lax.broadcasted_iota(jnp.int32, (1, 128), 1)
        row = row + jnp.where(lane == 8, summed(first), 0.0)
    return jnp.concatenate([row, jnp.zeros((7, 128), F32)], axis=0)


def misfit_body(iteration, first_ref, out_ref, x_ref, *refs):
    befores = refs[:iteration]
    row_ref, *kept = refs[iteration:]
    tokens, features = x_ref.shape
    sums = [jnp.zeros((8, 128), F32) for _ in range(iteration + 1)]
    first = jnp.zeros((8, 128), F32)
    for h in range(0, tokens, 16):
        at = slice(h, h + 16)
        image = first_ref[at, :features].astype(F32) + 0.5 * out_ref[at, :].astype(F32)
        misfit = image - x_ref[at, :]
        if kept:
            kept[0][at, :] = misfit
        for j in range(iteration + 1):
            other = misfit if j == iteration else befores[j][at, :]
            prod = folded_lanes(misfit * other)
            sums[j] = sums[j] + prod[:8] + prod[8:]
        if iteration == 1:
            prod = folded_lanes(befores[0][at, :] * befores[0][at, :])
            first = first + prod[:8] + prod[8:]
    row_ref[...] = gram_row(sums, first if iteration == 1 else None)


def last_misfit_body(inject_ref, *refs):
    outs, xs, row_ref = refs[: ITERS - 1], refs[ITERS - 1 : -1], refs[-1]
    inject = inject_ref[...].astype(F32)
    misfits = [xs[0][...]]
    for out_ref, x_ref in zip(outs, xs):
        misfits.append(inject + 0.5 * out_ref[...].astype(F32) - x_ref[...])
    row_ref[...] = gram_row([folded_lanes(misfits[-1] * m) for m in misfits], None)


def final_body(cells, rows_ref, inject_ref, start_ref, state_ref, *refs):
    outs, (x_ref, mix_ref) = refs[: ITERS - 1], refs[ITERS - 1 :]
    fresh = rows_ref[0:8]
    for h in range(8, rows_ref.shape[0], 8):
        fresh = fresh + rows_ref[h : h + 8]
    fresh = fresh[:, :128] + fresh[:, 128:]
    _, mix, entries = gram_and_weights(fresh, state_ref[...], ITERS - 1, cells)
    mix_ref[...] = weight_rows(mix, entries, False)
    inject = inject_ref[...].astype(F32)
    x = mix[0] * start_ref[...]
    for i in range(1, ITERS):
        x = x + mix[i] * (inject + 0.5 * outs[i - 1][...].astype(F32))
    x_ref[...] = x


def local(inject, w_gate, w_up, w_down, gain):
    rows, features = inject.shape[1:]
    sections = lax.axis_size("section")
    groups = lax.axis_size("dp")
    chips = groups // 2
    tokens = rows * chips
    cells = float(rows * groups * features)
    hidden = w_gate.shape[2]
    order = RING if chips == len(RING) else tuple(range(chips))
    same_core = [[2 * h + c for h in order] for c in range(2)]
    across = [(d, d ^ 1) for d in range(groups)]
    ahead = [(s, (s + 1) % sections) for s in range(sections)]
    ahead_across = [
        (s * groups + d, (s + 1) % sections * groups + (d ^ 1))
        for s in range(sections)
        for d in range(groups)
    ]
    both = ("section", "dp")

    def to_chips(array):
        return lax.all_to_all(array, "dp", 0, 0, tiled=True, axis_index_groups=same_core)

    def to_all(block):
        wider = jnp.broadcast_to(block[None], (chips, *block.shape))
        return to_chips(wider).reshape(chips * block.shape[0], block.shape[1])

    shape = jax.ShapeDtypeStruct
    mine = inject[0]
    mine_w = [w_gate[0].T, w_up[0].T, w_down[0]]
    held = [pltpu.VMEM(w.shape, BF16) for w in mine_w] + [pltpu.SemaphoreType.DMA((3,))]
    near_far = [pl.BlockSpec(memory_space=pltpu.VMEM)]
    near_far += [pl.BlockSpec(memory_space=pltpu.HBM)] * 3
    part0 = pallas(start_body, shape((8, features // 8), BF16), "start", 60, held, near_far)(
        gain, *mine_w
    )
    part0, sent_w = lax.optimization_barrier((part0, mine_w))
    other_w = [lax.ppermute(w, "dp", across) for w in sent_w]
    near = lax.ppermute(part0, "section", ahead)
    far = lax.ppermute(part0, both, ahead_across)
    start_part = (near.astype(F32) + far.astype(F32)).astype(BF16)
    first = to_all(jnp.concatenate([mine, start_part], axis=1))

    part_shape = shape((tokens, features), BF16)
    wide_shape = shape((tokens, features), F32)
    own_shape = shape((rows, features), F32)
    small = shape((8, 128), F32)
    scratch = [pltpu.VMEM((tokens, features), BF16)]
    weights = mine_w + other_w
    misfits, gathered, own_outs, own_xs, mixing = [], [], [], [], []
    state = row = None
    for iteration in range(1, ITERS):
        if iteration == 1:
            body = functools.partial(first_block_body, order)
            shapes = (part_shape, wide_shape, own_shape)
            part, x, own_x = pallas(body, shapes, "block1", 12, scratch)(first, gain, *weights)
            misfits.append(x)
        else:
            body = functools.partial(block_body, iteration, cells, order)
            carried = [] if state is None else [state]
            other_row = lax.ppermute(row, "dp", across)
            shapes = [part_shape, own_shape, small, small]
            held = list(scratch)
            if iteration < ITERS - 1:
                shapes.append(wide_shape)
            else:
                held.append(pltpu.VMEM((tokens, features), F32))
            part, own_x, state, mix, *rest = pallas(body, shapes, f"block{iteration}", 12, held)(
                row, other_row, first, *gathered, *carried, gain, *weights
            )
            x = rest[0] if rest else None
            if iteration == 2:
                mixing.append(mix[1, :HIST])
            mixing.append(mix[0, :HIST])
        own_xs.append(own_x)
        total = jnp.sum(to_chips(part.reshape(chips, rows, features)).astype(F32), axis=0)
        before = lax.ppermute((own_xs[-1] + total).astype(BF16), "section", ahead)
        own_outs.append(before)
        if iteration < ITERS - 1:
            gathered.append(to_all(before))
            shapes = [small] + [wide_shape] * (iteration < ITERS - 2)
            row, *misfit = pallas(
                functools.partial(misfit_body, iteration), shapes, f"misfit{iteration}", 12
            )(first, gathered[-1], x, *misfits)
            misfits += misfit
    row = pallas(last_misfit_body, small, "last_misfit", 8)(mine, *own_outs, *own_xs)
    sums = to_all(jnp.concatenate([row, lax.ppermute(row, "dp", across)], axis=1))
    iterate, mix = pallas(functools.partial(final_body, cells), (own_shape, small), "final", 8)(
        sums, mine, own_xs[0], state, *own_outs
    )
    mixing.append(mix[0, :HIST])
    return iterate[None], jnp.stack(mixing)[None]


def solution(mesh):
    placed = (
        P("section", "dp", None),
        P("section", None, "dp"),
        P("section", None, "dp"),
        P("section", "dp", None),
        P("section", None),
    )
    return jax.shard_map(
        local,
        mesh=mesh,
        in_specs=placed,
        out_specs=(P("section", "dp", None), P("section", None, None)),
        check_vma=False,
    )
```

```python
import functools

import jax
import jax.numpy as jnp
from jax import lax
from jax.experimental import pallas as pl
from jax.experimental.pallas import tpu as pltpu
from jax.sharding import PartitionSpec as P

ITERS = 5
HIST = 5
F32 = jnp.float32
BF16 = jnp.bfloat16


MIB = 1024 * 1024
RING = tuple(
    4 * x + y
    for x, y in ((0, 0), (0, 1), (0, 2), (0, 3), (1, 3), (1, 2), (1, 1), (2, 1))
    + ((2, 2), (2, 3), (3, 3), (3, 2), (3, 1), (3, 0), (2, 0), (1, 0))
)


def pallas(body, out_shape, name, limit, scratch=(), cost=None):
    return pl.pallas_call(
        body,
        out_shape=out_shape,
        scratch_shapes=list(scratch),
        name=name,
        cost_estimate=cost,
        compiler_params=pltpu.CompilerParams(vmem_limit_bytes=limit * MIB),
    )


def silu_times(gate, up):
    return gate / (1.0 + jnp.exp(-gate)) * up


def normalized(values, gain):
    mean = jnp.mean(values * values, axis=-1, keepdims=True)
    return (values * lax.rsqrt(mean + 1e-06) * gain).astype(BF16)


def by_rows(a, b):
    return lax.dot_general(a, b, (((1,), (1,)), ((), ())), preferred_element_type=F32)


def start_body(gain_ref, gate_ref, up_ref, down_ref, part_ref):
    features = gate_ref.shape[1]
    normed = normalized(jnp.zeros((8, features), F32), gain_ref[...])
    gate = by_rows(normed, gate_ref[...])
    up = by_rows(normed, up_ref[...])
    act = silu_times(gate, up).astype(BF16)
    piece = features // 8
    row = lax.broadcasted_iota(jnp.int32, (8, piece), 0)
    folded = jnp.zeros((8, piece), F32)
    for r in range(8):
        out = jnp.dot(act, down_ref[:, r * piece : (r + 1) * piece], preferred_element_type=F32)
        folded = folded + jnp.where(row == r, out, 0.0)
    part_ref[...] = folded.astype(BF16)


def entry(row, lane):
    return row[:, lane : lane + 1]


def solved_weights(entries, iteration):
    count = iteration + 1
    trace = entries[0][0]
    for i in range(1, count):
        trace = trace + entries[i][i]
    damp = 0.01 * trace / count + 1e-06
    rows = [[entries[i][j] for j in range(count)] for i in range(count)]
    for i in range(count):
        rows[i][i] = rows[i][i] + damp
    values = [jnp.ones((1, 1), F32) for _ in range(count)]
    for p in range(count):
        for i in range(p + 1, count):
            factor = rows[i][p] / rows[p][p]
            for j in range(p, count):
                rows[i][j] = rows[i][j] - factor * rows[p][j]
            values[i] = values[i] - factor * values[p]
    beta = [None] * count
    for i in range(count - 1, -1, -1):
        accum = values[i]
        for j in range(i + 1, count):
            accum = accum - rows[i][j] * beta[j]
        beta[i] = accum / rows[i][i]
    total = beta[0]
    for i in range(1, count):
        total = total + beta[i]
    return [b / total for b in beta]


def lane_row(values):
    lane = lax.broadcasted_iota(jnp.int32, (1, 128), 1)
    out = jnp.zeros((1, 128), F32)
    for j, value in enumerate(values):
        out = out + jnp.where(lane == j, value, 0.0)
    return out


def gram_and_weights(fresh, state, iteration, cells):
    fresh = fresh[0:1] / cells
    if state is None:
        known = [lane_row([entry(fresh, 8)]), fresh]
    else:
        known = [state[i : i + 1] for i in range(iteration)] + [fresh]
    entries = [[None] * (iteration + 1) for _ in range(iteration + 1)]
    for i in range(iteration + 1):
        for j in range(i + 1):
            entries[i][j] = entries[j][i] = entry(known[i], j)
    weights = solved_weights(entries, iteration)
    kept = known + [jnp.zeros((8 - len(known), 128), F32)]
    return jnp.concatenate(kept, axis=0), weights, entries


def weight_rows(weights, entries, first):
    rows = [lane_row(weights)]
    if first:
        rows.append(lane_row(solved_weights(entries, 0)))
    rows.append(jnp.zeros((8 - len(rows), 128), F32))
    return jnp.concatenate(rows, axis=0)


def start_row(first_ref, features):
    tokens = first_ref.shape[0]
    sums = first_ref[0:8, features:].astype(F32)
    for h in range(1, tokens // 8):
        sums = sums + first_ref[8 * h : 8 * h + 8, features:].astype(F32)
    sums = sums.astype(BF16).astype(F32)
    return jnp.concatenate([sums[r : r + 1] for r in range(8)], axis=1)


def products(rows_ref, weights, pre_ref):
    for i, w_ref in enumerate(weights):
        hidden = w_ref.shape[0]
        pre_ref[i * hidden : (i + 1) * hidden] = by_rows(w_ref[...], rows_ref[...])


def products_body(rows_ref, *refs):
    products(rows_ref, refs[:4], refs[4])


def lane_rsqrt(squares_ref, features):
    mean = jnp.transpose(squares_ref[...])[:1] * (1.0 / features)
    return lax.rsqrt(mean + 1e-06)


def squares_of(rows):
    sums = jnp.sum(rows * rows, axis=1, keepdims=True)
    return jnp.broadcast_to(sums, (rows.shape[0], 128))


def send_block(pre, factor, downs, part_ref):
    hidden = downs[0].shape[0]
    acts = []
    for half in range(2):
        gate = pre(2 * half * hidden, hidden) * factor
        up = pre((2 * half + 1) * hidden, hidden) * factor
        acts.append(jnp.transpose(silu_times(gate, up)).astype(BF16))
    features = part_ref.shape[1]
    step = min(512, features)
    for n in range(0, features, step):
        cols = slice(n, n + step)
        part = jnp.dot(acts[0], downs[0][:, cols], preferred_element_type=F32)
        part = part + jnp.dot(acts[1], downs[1][:, cols], preferred_element_type=F32)
        part_ref[:, cols] = part.astype(BF16)


def own_rows(x_ref, order):
    chip = lax.axis_index("dp") // 2
    slot = jnp.int32(0)
    for i, h in enumerate(order):
        slot = jnp.where(chip == h, i, slot)
    return x_ref[pl.ds(pl.multiple_of(8 * slot, 8), 8), :]


def first_block_body(order, first_ref, gain_ref, *refs):
    weights, downs = refs[:4], refs[4:6]
    part_ref, x_ref, own_x_ref, pre_ref, scaled_ref, squares_ref = refs[6:]
    tokens, features = part_ref.shape
    half = 0.5 * start_row(first_ref, features)
    for h in range(0, tokens, 16):
        rows = first_ref[h : h + 16, :features].astype(F32) + half
        x_ref[h : h + 16, :] = rows
        scaled_ref[h : h + 16, :] = (rows * gain_ref[...]).astype(BF16)
        squares_ref[h : h + 16, :] = squares_of(rows)
    own_x_ref[...] = own_rows(x_ref, order)
    products(scaled_ref, weights, pre_ref)
    factor = lane_rsqrt(squares_ref, features)
    send_block(lambda at, size: pre_ref[at : at + size], factor, downs, part_ref)


def block_body(iteration, cells, order, *refs):
    own_ref, other_ref, first_ref = refs[:3]
    outs = refs[3 : 2 + iteration]
    pres = refs[2 + iteration : 2 + 2 * iteration]
    at = 2 + 2 * iteration
    state = None
    if iteration > 2:
        state = refs[at][...]
        at += 1
    downs = refs[at : at + 2]
    if iteration < ITERS - 1:
        part_ref, own_x_ref, kept_ref, mix_ref, x_ref, squares_ref = refs[at + 2 :]
    else:
        part_ref, own_x_ref, kept_ref, mix_ref, squares_ref, x_ref = refs[at + 2 :]
    tokens, features = part_ref.shape
    fresh = own_ref[...] + other_ref[...]
    kept, mix, entries = gram_and_weights(fresh, state, iteration - 1, cells)
    kept_ref[...] = kept
    mix_ref[...] = weight_rows(mix, entries, iteration == 2)
    total = mix[0]
    for i in range(1, iteration):
        total = total + mix[i]
    base = (0.5 * mix[0]) * start_row(first_ref, features)
    for h in range(0, tokens, 16):
        rows = total * first_ref[h : h + 16, :features].astype(F32) + base
        for i in range(1, iteration):
            rows = rows + (0.5 * mix[i]) * outs[i - 1][h : h + 16, :].astype(F32)
        x_ref[h : h + 16, :] = rows
        squares_ref[h : h + 16, :] = squares_of(rows)
    own_x_ref[...] = own_rows(x_ref, order)
    factor = lane_rsqrt(squares_ref, features)

    def mixed(start, size):
        accum = mix[0] * pres[0][start : start + size]
        for i in range(1, iteration):
            accum = accum + mix[i] * pres[i][start : start + size]
        return accum

    send_block(mixed, factor, downs, part_ref)


def folded_lanes(values):
    pieces = [values[:, n : n + 128] for n in range(0, values.shape[1], 128)]
    while len(pieces) > 1:
        pieces = [a + b for a, b in zip(pieces[::2], pieces[1::2])]
    return pieces[0]


def summed(values):
    return jnp.sum(jnp.sum(values, axis=0, keepdims=True), axis=1, keepdims=True)


def gram_row(sums, first):
    row = lane_row([summed(s) for s in sums])
    if first is not None:
        lane = lax.broadcasted_iota(jnp.int32, (1, 128), 1)
        row = row + jnp.where(lane == 8, summed(first), 0.0)
    return jnp.concatenate([row, jnp.zeros((7, 128), F32)], axis=0)


def misfit_body(iteration, first_ref, out_ref, x_ref, gain_ref, *refs):
    befores = refs[:iteration]
    row_ref, scaled_ref, *kept = refs[iteration:]
    tokens, features = x_ref.shape
    sums = [jnp.zeros((8, 128), F32) for _ in range(iteration + 1)]
    first = jnp.zeros((8, 128), F32)
    for h in range(0, tokens, 16):
        at = slice(h, h + 16)
        image = first_ref[at, :features].astype(F32) + 0.5 * out_ref[at, :].astype(F32)
        scaled_ref[at, :] = (image * gain_ref[...]).astype(BF16)
        misfit = image - x_ref[at, :]
        if kept:
            kept[0][at, :] = misfit
        for j in range(iteration + 1):
            other = misfit if j == iteration else befores[j][at, :]
            prod = folded_lanes(misfit * other)
            sums[j] = sums[j] + prod[:8] + prod[8:]
        if iteration == 1:
            prod = folded_lanes(befores[0][at, :] * befores[0][at, :])
            first = first + prod[:8] + prod[8:]
    row_ref[...] = gram_row(sums, first if iteration == 1 else None)


def last_misfit_body(inject_ref, *refs):
    outs, xs, row_ref = refs[: ITERS - 1], refs[ITERS - 1 : -1], refs[-1]
    inject = inject_ref[...].astype(F32)
    misfits = [xs[0][...]]
    for out_ref, x_ref in zip(outs, xs):
        misfits.append(inject + 0.5 * out_ref[...].astype(F32) - x_ref[...])
    row_ref[...] = gram_row([folded_lanes(misfits[-1] * m) for m in misfits], None)


def final_body(cells, rows_ref, inject_ref, start_ref, state_ref, *refs):
    outs, (x_ref, mix_ref) = refs[: ITERS - 1], refs[ITERS - 1 :]
    fresh = rows_ref[0:8]
    for h in range(8, rows_ref.shape[0], 8):
        fresh = fresh + rows_ref[h : h + 8]
    _, mix, entries = gram_and_weights(fresh, state_ref[...], ITERS - 1, cells)
    mix_ref[...] = weight_rows(mix, entries, False)
    inject = inject_ref[...].astype(F32)
    x = mix[0] * start_ref[...]
    for i in range(1, ITERS):
        x = x + mix[i] * (inject + 0.5 * outs[i - 1][...].astype(F32))
    x_ref[...] = x


def local(inject, w_gate, w_up, w_down, gain):
    rows, features = inject.shape[1:]
    sections = lax.axis_size("section")
    groups = lax.axis_size("dp")
    chips = groups // 2
    tokens = rows * chips
    cells = float(rows * groups * features)
    hidden = w_gate.shape[2]
    order = RING if chips == len(RING) else tuple(range(chips))
    same_core = [[2 * h + c for h in order] for c in range(2)]
    across = [(d, d ^ 1) for d in range(groups)]
    ahead = [(s, (s + 1) % sections) for s in range(sections)]
    ahead_across = [
        (s * groups + d, (s + 1) % sections * groups + (d ^ 1))
        for s in range(sections)
        for d in range(groups)
    ]
    both = ("section", "dp")

    def to_chips(array):
        return lax.all_to_all(array, "dp", 0, 0, tiled=True, axis_index_groups=same_core)

    def to_all(block):
        wider = jnp.broadcast_to(block[None], (chips, *block.shape))
        return to_chips(wider).reshape(chips * block.shape[0], block.shape[1])

    shape = jax.ShapeDtypeStruct
    mine = inject[0]
    mine_w = [w_gate[0].T, w_up[0].T, w_down[0]]
    part0 = pallas(start_body, shape((8, features // 8), BF16), "start", 12)(gain, *mine_w)
    other_w = [lax.ppermute(w, "dp", across) for w in mine_w]
    near = lax.ppermute(part0, "section", ahead)
    far = lax.ppermute(part0, both, ahead_across)
    start_part = (near.astype(F32) + far.astype(F32)).astype(BF16)
    first = to_all(jnp.concatenate([mine, start_part], axis=1))

    part_shape = shape((tokens, features), BF16)
    wide_shape = shape((tokens, features), F32)
    own_shape = shape((rows, features), F32)
    small = shape((8, 128), F32)
    scaled_shape = shape((tokens, features), BF16)
    pre_shape = shape((4 * hidden, tokens), F32)
    squares = pltpu.VMEM((tokens, 128), F32)
    weights = [mine_w[0], mine_w[1], other_w[0], other_w[1]]
    downs = [mine_w[2], other_w[2]]
    pres = []
    cost = pl.CostEstimate(
        flops=8 * hidden * tokens * features,
        bytes_accessed=8 * hidden * features,
        transcendentals=0,
    )
    misfits, gathered, own_outs, own_xs, mixing = [], [], [], [], []
    state = row = None
    for iteration in range(1, ITERS):
        if iteration == 1:
            body = functools.partial(first_block_body, order)
            shapes = (part_shape, wide_shape, own_shape, pre_shape)
            held = [pltpu.VMEM((tokens, features), BF16), squares]
            part, x, own_x, pre = pallas(body, shapes, "block1", 12, held)(
                first, gain, *weights, *downs
            )
            pres.append(pre)
            misfits.append(x)
        else:
            body = functools.partial(block_body, iteration, cells, order)
            carried = [] if state is None else [state]
            other_row = lax.ppermute(row, "dp", across)
            pres.append(
                pallas(products_body, pre_shape, f"products{iteration}", 12, cost=cost)(
                    scaled, *weights
                )
            )
            shapes = [part_shape, own_shape, small, small]
            held = [squares]
            if iteration < ITERS - 1:
                shapes.append(wide_shape)
            else:
                held.append(pltpu.VMEM((tokens, features), F32))
            part, own_x, state, mix, *rest = pallas(body, shapes, f"block{iteration}", 12, held)(
                row, other_row, first, *gathered, *pres, *carried, *downs
            )
            x = rest[0] if rest else None
            if iteration == 2:
                mixing.append(mix[1, :HIST])
            mixing.append(mix[0, :HIST])
        own_xs.append(own_x)
        total = jnp.sum(to_chips(part.reshape(chips, rows, features)).astype(F32), axis=0)
        before = lax.ppermute((own_xs[-1] + total).astype(BF16), "section", ahead)
        own_outs.append(before)
        if iteration < ITERS - 1:
            gathered.append(to_all(before))
            shapes = [small, scaled_shape] + [wide_shape] * (iteration < ITERS - 2)
            row, scaled, *misfit = pallas(
                functools.partial(misfit_body, iteration), shapes, f"misfit{iteration}", 12
            )(first, gathered[-1], x, gain, *misfits)
            misfits += misfit
    row = pallas(last_misfit_body, small, "last_misfit", 8)(mine, *own_outs, *own_xs)
    copies = jnp.broadcast_to(row[None], (groups, *row.shape))
    sums = lax.all_to_all(copies, "dp", 0, 0, tiled=True).reshape(8 * groups, 128)
    iterate, mix = pallas(functools.partial(final_body, cells), (own_shape, small), "final", 8)(
        sums, mine, own_xs[0], state, *own_outs
    )
    mixing.append(mix[0, :HIST])
    return iterate[None], jnp.stack(mixing)[None]


def solution(mesh):
    placed = (
        P("section", "dp", None),
        P("section", None, "dp"),
        P("section", None, "dp"),
        P("section", "dp", None),
        P("section", None),
    )
    return jax.shard_map(
        local,
        mesh=mesh,
        in_specs=placed,
        out_specs=(P("section", "dp", None), P("section", None, None)),
        check_vma=False,
    )
```

```python
import functools

import jax
import jax.numpy as jnp
from jax import lax
from jax.experimental import pallas as pl
from jax.experimental.pallas import tpu as pltpu
from jax.sharding import PartitionSpec as P

ITERS = 5
HIST = 5
F32 = jnp.float32
BF16 = jnp.bfloat16


MIB = 1024 * 1024
STAGGER = 1200
RING = tuple(
    4 * x + y
    for x, y in ((0, 0), (0, 1), (0, 2), (0, 3), (1, 3), (1, 2), (1, 1), (2, 1))
    + ((2, 2), (2, 3), (3, 3), (3, 2), (3, 1), (3, 0), (2, 0), (1, 0))
)


def pallas(body, out_shape, name, limit, scratch=(), cost=None):
    return pl.pallas_call(
        body,
        out_shape=out_shape,
        scratch_shapes=list(scratch),
        name=name,
        cost_estimate=cost,
        compiler_params=pltpu.CompilerParams(vmem_limit_bytes=limit * MIB),
    )


def silu_times(gate, up):
    return gate / (1.0 + jnp.exp(-gate)) * up


def normalized(values, gain):
    mean = jnp.mean(values * values, axis=-1, keepdims=True)
    return (values * lax.rsqrt(mean + 1e-06) * gain).astype(BF16)


def by_rows(a, b):
    return lax.dot_general(a, b, (((1,), (1,)), ((), ())), preferred_element_type=F32)


def start_body(gain_ref, gate_ref, up_ref, down_ref, part_ref):
    features = gate_ref.shape[1]
    normed = normalized(jnp.zeros((8, features), F32), gain_ref[...])
    gate = by_rows(normed, gate_ref[...])
    up = by_rows(normed, up_ref[...])
    act = silu_times(gate, up).astype(BF16)
    piece = features // 8
    row = lax.broadcasted_iota(jnp.int32, (8, piece), 0)
    folded = jnp.zeros((8, piece), F32)
    for r in range(8):
        out = jnp.dot(act, down_ref[:, r * piece : (r + 1) * piece], preferred_element_type=F32)
        folded = folded + jnp.where(row == r, out, 0.0)
    part_ref[...] = folded.astype(BF16)


def entry(row, lane):
    return row[:, lane : lane + 1]


def solved_weights(entries, iteration):
    count = iteration + 1
    trace = entries[0][0]
    for i in range(1, count):
        trace = trace + entries[i][i]
    damp = 0.01 * trace / count + 1e-06
    rows = [[entries[i][j] for j in range(count)] for i in range(count)]
    for i in range(count):
        rows[i][i] = rows[i][i] + damp
    values = [jnp.ones((1, 1), F32) for _ in range(count)]
    for p in range(count):
        for i in range(p + 1, count):
            factor = rows[i][p] / rows[p][p]
            for j in range(p, count):
                rows[i][j] = rows[i][j] - factor * rows[p][j]
            values[i] = values[i] - factor * values[p]
    beta = [None] * count
    for i in range(count - 1, -1, -1):
        accum = values[i]
        for j in range(i + 1, count):
            accum = accum - rows[i][j] * beta[j]
        beta[i] = accum / rows[i][i]
    total = beta[0]
    for i in range(1, count):
        total = total + beta[i]
    return [b / total for b in beta]


def lane_row(values):
    lane = lax.broadcasted_iota(jnp.int32, (1, 128), 1)
    out = jnp.zeros((1, 128), F32)
    for j, value in enumerate(values):
        out = out + jnp.where(lane == j, value, 0.0)
    return out


def gram_and_weights(fresh, state, iteration, cells):
    fresh = fresh[0:1] / cells
    if state is None:
        known = [lane_row([entry(fresh, 8)]), fresh]
    else:
        known = [state[i : i + 1] for i in range(iteration)] + [fresh]
    entries = [[None] * (iteration + 1) for _ in range(iteration + 1)]
    for i in range(iteration + 1):
        for j in range(i + 1):
            entries[i][j] = entries[j][i] = entry(known[i], j)
    weights = solved_weights(entries, iteration)
    kept = known + [jnp.zeros((8 - len(known), 128), F32)]
    return jnp.concatenate(kept, axis=0), weights, entries


def weight_rows(weights, entries, first):
    rows = [lane_row(weights)]
    if first:
        rows.append(lane_row(solved_weights(entries, 0)))
    rows.append(jnp.zeros((8 - len(rows), 128), F32))
    return jnp.concatenate(rows, axis=0)


def start_row(first_ref, features):
    tokens = first_ref.shape[0]
    sums = first_ref[0:8, features:].astype(F32)
    for h in range(1, tokens // 8):
        sums = sums + first_ref[8 * h : 8 * h + 8, features:].astype(F32)
    sums = sums.astype(BF16).astype(F32)
    return jnp.concatenate([sums[r : r + 1] for r in range(8)], axis=1)


def products(rows_ref, weights, pre_ref):
    for i, w_ref in enumerate(weights):
        hidden = w_ref.shape[0]
        pre_ref[i * hidden : (i + 1) * hidden] = by_rows(w_ref[...], rows_ref[...])


def products_body(rows_ref, *refs):
    products(rows_ref, refs[:4], refs[4])


def lane_rsqrt(squares_ref, features):
    mean = jnp.transpose(squares_ref[...])[:1] * (1.0 / features)
    return lax.rsqrt(mean + 1e-06)


def squares_of(rows):
    sums = jnp.sum(rows * rows, axis=1, keepdims=True)
    return jnp.broadcast_to(sums, (rows.shape[0], 128))


def send_block(pre, factor, downs, part_ref):
    hidden = downs[0].shape[0]
    acts = []
    for half in range(2):
        gate = pre(2 * half * hidden, hidden) * factor
        up = pre((2 * half + 1) * hidden, hidden) * factor
        acts.append(jnp.transpose(silu_times(gate, up)).astype(BF16))
    features = part_ref.shape[1]
    step = min(512, features)
    for n in range(0, features, step):
        cols = slice(n, n + step)
        part = jnp.dot(acts[0], downs[0][:, cols], preferred_element_type=F32)
        part = part + jnp.dot(acts[1], downs[1][:, cols], preferred_element_type=F32)
        part_ref[:, cols] = part.astype(BF16)


def own_rows(x_ref, order):
    chip = lax.axis_index("dp") // 2
    slot = jnp.int32(0)
    for i, h in enumerate(order):
        slot = jnp.where(chip == h, i, slot)
    return x_ref[pl.ds(pl.multiple_of(8 * slot, 8), 8), :]


def first_block_body(order, first_ref, gain_ref, *refs):
    weights, downs = refs[:4], refs[4:6]
    part_ref, x_ref, own_x_ref, pre_ref, scaled_ref, squares_ref = refs[6:]
    tokens, features = part_ref.shape
    half = 0.5 * start_row(first_ref, features)
    for h in range(0, tokens, 16):
        rows = first_ref[h : h + 16, :features].astype(F32) + half
        x_ref[h : h + 16, :] = rows
        scaled_ref[h : h + 16, :] = (rows * gain_ref[...]).astype(BF16)
        squares_ref[h : h + 16, :] = squares_of(rows)
    own_x_ref[...] = own_rows(x_ref, order)
    products(scaled_ref, weights, pre_ref)
    factor = lane_rsqrt(squares_ref, features)
    send_block(lambda at, size: pre_ref[at : at + size], factor, downs, part_ref)


def block_body(iteration, cells, order, *refs):
    own_ref, other_ref, first_ref = refs[:3]
    outs = refs[3 : 2 + iteration]
    pres = refs[2 + iteration : 2 + 2 * iteration]
    at = 2 + 2 * iteration
    state = None
    if iteration > 2:
        state = refs[at][...]
        at += 1
    downs = refs[at : at + 2]
    if iteration < ITERS - 1:
        part_ref, own_x_ref, kept_ref, mix_ref, x_ref, squares_ref = refs[at + 2 :]
    else:
        part_ref, own_x_ref, kept_ref, mix_ref, squares_ref, x_ref = refs[at + 2 :]
    tokens, features = part_ref.shape
    fresh = own_ref[...] + other_ref[...]
    kept, mix, entries = gram_and_weights(fresh, state, iteration - 1, cells)
    kept_ref[...] = kept
    mix_ref[...] = weight_rows(mix, entries, iteration == 2)
    total = mix[0]
    for i in range(1, iteration):
        total = total + mix[i]
    base = (0.5 * mix[0]) * start_row(first_ref, features)
    for h in range(0, tokens, 16):
        rows = total * first_ref[h : h + 16, :features].astype(F32) + base
        for i in range(1, iteration):
            rows = rows + (0.5 * mix[i]) * outs[i - 1][h : h + 16, :].astype(F32)
        x_ref[h : h + 16, :] = rows
        squares_ref[h : h + 16, :] = squares_of(rows)
    own_x_ref[...] = own_rows(x_ref, order)
    factor = lane_rsqrt(squares_ref, features)

    def mixed(start, size):
        accum = mix[0] * pres[0][start : start + size]
        for i in range(1, iteration):
            accum = accum + mix[i] * pres[i][start : start + size]
        return accum

    send_block(mixed, factor, downs, part_ref)

    if iteration < ITERS - 1:

        @pl.when(lax.axis_index("dp") % 2 == 1)
        def _():
            mix_ref[7:8] = lax.fori_loop(0, STAGGER, lambda _, v: v * 0.5 + 0.5, mix_ref[7:8])


def folded_lanes(values):
    pieces = [values[:, n : n + 128] for n in range(0, values.shape[1], 128)]
    while len(pieces) > 1:
        pieces = [a + b for a, b in zip(pieces[::2], pieces[1::2])]
    return pieces[0]


def summed(values):
    return jnp.sum(jnp.sum(values, axis=0, keepdims=True), axis=1, keepdims=True)


def gram_row(sums, first):
    row = lane_row([summed(s) for s in sums])
    if first is not None:
        lane = lax.broadcasted_iota(jnp.int32, (1, 128), 1)
        row = row + jnp.where(lane == 8, summed(first), 0.0)
    return jnp.concatenate([row, jnp.zeros((7, 128), F32)], axis=0)


def misfit_body(iteration, first_ref, out_ref, x_ref, gain_ref, *refs):
    befores = refs[:iteration]
    row_ref, scaled_ref, *kept = refs[iteration:]
    tokens, features = x_ref.shape
    sums = [jnp.zeros((8, 128), F32) for _ in range(iteration + 1)]
    first = jnp.zeros((8, 128), F32)
    for h in range(0, tokens, 16):
        at = slice(h, h + 16)
        image = first_ref[at, :features].astype(F32) + 0.5 * out_ref[at, :].astype(F32)
        scaled_ref[at, :] = (image * gain_ref[...]).astype(BF16)
        misfit = image - x_ref[at, :]
        if kept:
            kept[0][at, :] = misfit
        for j in range(iteration + 1):
            other = misfit if j == iteration else befores[j][at, :]
            prod = folded_lanes(misfit * other)
            sums[j] = sums[j] + prod[:8] + prod[8:]
        if iteration == 1:
            prod = folded_lanes(befores[0][at, :] * befores[0][at, :])
            first = first + prod[:8] + prod[8:]
    row_ref[...] = gram_row(sums, first if iteration == 1 else None)


def last_misfit_body(inject_ref, *refs):
    outs, xs, row_ref = refs[: ITERS - 1], refs[ITERS - 1 : -1], refs[-1]
    inject = inject_ref[...].astype(F32)
    misfits = [xs[0][...]]
    for out_ref, x_ref in zip(outs, xs):
        misfits.append(inject + 0.5 * out_ref[...].astype(F32) - x_ref[...])
    row_ref[...] = gram_row([folded_lanes(misfits[-1] * m) for m in misfits], None)


def final_body(cells, rows_ref, inject_ref, start_ref, state_ref, *refs):
    outs, (x_ref, mix_ref) = refs[: ITERS - 1], refs[ITERS - 1 :]
    fresh = rows_ref[0:8]
    for h in range(8, rows_ref.shape[0], 8):
        fresh = fresh + rows_ref[h : h + 8]
    _, mix, entries = gram_and_weights(fresh, state_ref[...], ITERS - 1, cells)
    mix_ref[...] = weight_rows(mix, entries, False)
    inject = inject_ref[...].astype(F32)
    x = mix[0] * start_ref[...]
    for i in range(1, ITERS):
        x = x + mix[i] * (inject + 0.5 * outs[i - 1][...].astype(F32))
    x_ref[...] = x


def local(inject, w_gate, w_up, w_down, gain):
    rows, features = inject.shape[1:]
    sections = lax.axis_size("section")
    groups = lax.axis_size("dp")
    chips = groups // 2
    tokens = rows * chips
    cells = float(rows * groups * features)
    hidden = w_gate.shape[2]
    order = RING if chips == len(RING) else tuple(range(chips))
    same_core = [[2 * h + c for h in order] for c in range(2)]
    across = [(d, d ^ 1) for d in range(groups)]
    ahead = [(s, (s + 1) % sections) for s in range(sections)]
    def to_chips(array):
        return lax.all_to_all(array, "dp", 0, 0, tiled=True, axis_index_groups=same_core)

    def to_all(block):
        wider = jnp.broadcast_to(block[None], (chips, *block.shape))
        return to_chips(wider).reshape(chips * block.shape[0], block.shape[1])

    shape = jax.ShapeDtypeStruct
    mine = inject[0]
    mine_w = [w_gate[0].T, w_up[0].T, w_down[0]]
    part0 = pallas(start_body, shape((8, features // 8), BF16), "start", 12)(gain, *mine_w)
    other_w = [lax.ppermute(w, "dp", across) for w in mine_w]
    other0 = lax.ppermute(part0, "dp", across)
    pair0 = (part0.astype(F32) + other0.astype(F32)).astype(BF16)
    start_part = lax.ppermute(pair0, "section", ahead)
    first = to_all(jnp.concatenate([mine, start_part], axis=1))

    part_shape = shape((tokens, features), BF16)
    wide_shape = shape((tokens, features), F32)
    own_shape = shape((rows, features), F32)
    small = shape((8, 128), F32)
    scaled_shape = shape((tokens, features), BF16)
    pre_shape = shape((4 * hidden, tokens), F32)
    squares = pltpu.VMEM((tokens, 128), F32)
    weights = [mine_w[0], mine_w[1], other_w[0], other_w[1]]
    downs = [mine_w[2], other_w[2]]
    pres = []
    cost = pl.CostEstimate(
        flops=8 * hidden * tokens * features,
        bytes_accessed=8 * hidden * features,
        transcendentals=0,
    )
    misfits, gathered, own_outs, own_xs, mixing = [], [], [], [], []
    state = row = None
    for iteration in range(1, ITERS):
        if iteration == 1:
            body = functools.partial(first_block_body, order)
            shapes = (part_shape, wide_shape, own_shape, pre_shape)
            held = [pltpu.VMEM((tokens, features), BF16), squares]
            part, x, own_x, pre = pallas(body, shapes, "block1", 12, held)(
                first, gain, *weights, *downs
            )
            pres.append(pre)
            misfits.append(x)
        else:
            body = functools.partial(block_body, iteration, cells, order)
            carried = [] if state is None else [state]
            other_row = lax.ppermute(row, "dp", across)
            pres.append(
                pallas(products_body, pre_shape, f"products{iteration}", 12, cost=cost)(
                    scaled, *weights
                )
            )
            shapes = [part_shape, own_shape, small, small]
            held = [squares]
            if iteration < ITERS - 1:
                shapes.append(wide_shape)
            else:
                held.append(pltpu.VMEM((tokens, features), F32))
            part, own_x, state, mix, *rest = pallas(body, shapes, f"block{iteration}", 12, held)(
                row, other_row, first, *gathered, *pres, *carried, *downs
            )
            x = rest[0] if rest else None
            if iteration == 2:
                mixing.append(mix[1, :HIST])
            mixing.append(mix[0, :HIST])
        own_xs.append(own_x)
        total = jnp.sum(to_chips(part.reshape(chips, rows, features)).astype(F32), axis=0)
        before = lax.ppermute((own_xs[-1] + total).astype(BF16), "section", ahead)
        own_outs.append(before)
        if iteration < ITERS - 1:
            gathered.append(to_all(before))
            shapes = [small, scaled_shape] + [wide_shape] * (iteration < ITERS - 2)
            row, scaled, *misfit = pallas(
                functools.partial(misfit_body, iteration), shapes, f"misfit{iteration}", 12
            )(first, gathered[-1], x, gain, *misfits)
            misfits += misfit
    row = pallas(last_misfit_body, small, "last_misfit", 8)(mine, *own_outs, *own_xs)
    copies = jnp.broadcast_to(row[None], (groups, *row.shape))
    sums = lax.all_to_all(copies, "dp", 0, 0, tiled=True).reshape(8 * groups, 128)
    iterate, mix = pallas(functools.partial(final_body, cells), (own_shape, small), "final", 8)(
        sums, mine, own_xs[0], state, *own_outs
    )
    mixing.append(mix[0, :HIST])
    return iterate[None], jnp.stack(mixing)[None]


def solution(mesh):
    placed = (
        P("section", "dp", None),
        P("section", None, "dp"),
        P("section", None, "dp"),
        P("section", "dp", None),
        P("section", None),
    )
    return jax.shard_map(
        local,
        mesh=mesh,
        in_specs=placed,
        out_specs=(P("section", "dp", None), P("section", None, None)),
        check_vma=False,
    )
```

```python
import functools

import jax
import jax.numpy as jnp
from jax import lax
from jax.experimental import pallas as pl
from jax.experimental.pallas import tpu as pltpu
from jax.sharding import PartitionSpec as P

ITERS = 5
HIST = 5
F32 = jnp.float32
BF16 = jnp.bfloat16


MIB = 1024 * 1024
RING = tuple(
    4 * x + y
    for x, y in ((0, 0), (0, 1), (0, 2), (0, 3), (1, 3), (1, 2), (1, 1), (2, 1))
    + ((2, 2), (2, 3), (3, 3), (3, 2), (3, 1), (3, 0), (2, 0), (1, 0))
)


def pallas(body, out_shape, name, limit, scratch=(), cost=None):
    return pl.pallas_call(
        body,
        out_shape=out_shape,
        scratch_shapes=list(scratch),
        name=name,
        cost_estimate=cost,
        compiler_params=pltpu.CompilerParams(vmem_limit_bytes=limit * MIB),
    )


def silu_times(gate, up):
    return gate / (1.0 + jnp.exp(-gate)) * up


def normalized(values, gain):
    mean = jnp.mean(values * values, axis=-1, keepdims=True)
    return (values * lax.rsqrt(mean + 1e-06) * gain).astype(BF16)


def by_rows(a, b):
    return lax.dot_general(a, b, (((1,), (1,)), ((), ())), preferred_element_type=F32)


def start_body(gain_ref, gate_ref, up_ref, down_ref, part_ref):
    features = gate_ref.shape[1]
    normed = normalized(jnp.zeros((8, features), F32), gain_ref[...])
    gate = by_rows(normed, gate_ref[...])
    up = by_rows(normed, up_ref[...])
    act = silu_times(gate, up).astype(BF16)
    piece = features // 8
    row = lax.broadcasted_iota(jnp.int32, (8, piece), 0)
    folded = jnp.zeros((8, piece), F32)
    for r in range(8):
        out = jnp.dot(act, down_ref[:, r * piece : (r + 1) * piece], preferred_element_type=F32)
        folded = folded + jnp.where(row == r, out, 0.0)
    part_ref[...] = folded.astype(BF16)


def entry(row, lane):
    return row[:, lane : lane + 1]


def solved_weights(entries, iteration):
    count = iteration + 1
    trace = entries[0][0]
    for i in range(1, count):
        trace = trace + entries[i][i]
    damp = 0.01 * trace / count + 1e-06
    rows = [[entries[i][j] for j in range(count)] for i in range(count)]
    for i in range(count):
        rows[i][i] = rows[i][i] + damp
    values = [jnp.ones((1, 1), F32) for _ in range(count)]
    for p in range(count):
        for i in range(p + 1, count):
            factor = rows[i][p] / rows[p][p]
            for j in range(p, count):
                rows[i][j] = rows[i][j] - factor * rows[p][j]
            values[i] = values[i] - factor * values[p]
    beta = [None] * count
    for i in range(count - 1, -1, -1):
        accum = values[i]
        for j in range(i + 1, count):
            accum = accum - rows[i][j] * beta[j]
        beta[i] = accum / rows[i][i]
    total = beta[0]
    for i in range(1, count):
        total = total + beta[i]
    return [b / total for b in beta]


def lane_row(values):
    lane = lax.broadcasted_iota(jnp.int32, (1, 128), 1)
    out = jnp.zeros((1, 128), F32)
    for j, value in enumerate(values):
        out = out + jnp.where(lane == j, value, 0.0)
    return out


def gram_and_weights(fresh, state, iteration, cells):
    fresh = fresh[0:1] / cells
    if state is None:
        known = [lane_row([entry(fresh, 8)]), fresh]
    else:
        known = [state[i : i + 1] for i in range(iteration)] + [fresh]
    entries = [[None] * (iteration + 1) for _ in range(iteration + 1)]
    for i in range(iteration + 1):
        for j in range(i + 1):
            entries[i][j] = entries[j][i] = entry(known[i], j)
    weights = solved_weights(entries, iteration)
    kept = known + [jnp.zeros((8 - len(known), 128), F32)]
    return jnp.concatenate(kept, axis=0), weights, entries


def weight_rows(weights, entries, first):
    rows = [lane_row(weights)]
    if first:
        rows.append(lane_row(solved_weights(entries, 0)))
    rows.append(jnp.zeros((8 - len(rows), 128), F32))
    return jnp.concatenate(rows, axis=0)


def start_row(first_ref, features):
    tokens = first_ref.shape[0]
    sums = first_ref[0:8, features:].astype(F32)
    for h in range(1, tokens // 8):
        sums = sums + first_ref[8 * h : 8 * h + 8, features:].astype(F32)
    sums = sums.astype(BF16).astype(F32)
    return jnp.concatenate([sums[r : r + 1] for r in range(8)], axis=1)


def products(rows_ref, weights, pre_ref):
    for i, w_ref in enumerate(weights):
        hidden = w_ref.shape[0]
        pre_ref[i * hidden : (i + 1) * hidden] = by_rows(w_ref[...], rows_ref[...])


def on_core(core):
    return pl.when(lax.axis_index("dp") % 2 == core)


def products_body(rows_ref, *refs):
    @on_core(1)
    def _():
        products(rows_ref, refs[:4], refs[4])


def lane_rsqrt(squares_ref, features):
    mean = jnp.transpose(squares_ref[...])[:1] * (1.0 / features)
    return lax.rsqrt(mean + 1e-06)


def squares_of(rows):
    sums = jnp.sum(rows * rows, axis=1, keepdims=True)
    return jnp.broadcast_to(sums, (rows.shape[0], 128))


def send_block(pre, factor, downs, part_ref):
    hidden = downs[0].shape[0]
    acts = []
    for half in range(2):
        gate = pre(2 * half * hidden, hidden) * factor
        up = pre((2 * half + 1) * hidden, hidden) * factor
        acts.append(jnp.transpose(silu_times(gate, up)).astype(BF16))
    features = part_ref.shape[1]
    step = min(512, features)
    for n in range(0, features, step):
        cols = slice(n, n + step)
        part = jnp.dot(acts[0], downs[0][:, cols], preferred_element_type=F32)
        part = part + jnp.dot(acts[1], downs[1][:, cols], preferred_element_type=F32)
        part_ref[:, cols] = part.astype(BF16)


def own_rows(x_ref, order):
    chip = lax.axis_index("dp") // 2
    slot = jnp.int32(0)
    for i, h in enumerate(order):
        slot = jnp.where(chip == h, i, slot)
    return x_ref[pl.ds(pl.multiple_of(8 * slot, 8), 8), :]


def first_block_body(order, first_ref, gain_ref, *refs):
    weights, downs = refs[:4], refs[4:6]
    part_ref, x_ref, own_x_ref, pre_ref, scaled_ref, squares_ref = refs[6:]
    tokens, features = part_ref.shape
    half = 0.5 * start_row(first_ref, features)
    for h in range(0, tokens, 16):
        rows = first_ref[h : h + 16, :features].astype(F32) + half
        x_ref[h : h + 16, :] = rows
        scaled_ref[h : h + 16, :] = (rows * gain_ref[...]).astype(BF16)
        squares_ref[h : h + 16, :] = squares_of(rows)
    own_x_ref[...] = own_rows(x_ref, order)
    products(scaled_ref, weights, pre_ref)
    factor = lane_rsqrt(squares_ref, features)
    send_block(lambda at, size: pre_ref[at : at + size], factor, downs, part_ref)


def block_body(iteration, cells, order, *refs):
    own_ref, other_ref, first_ref = refs[:3]
    outs = refs[3 : 2 + iteration]
    ready_ref = refs[2 + iteration]
    pres = refs[3 + iteration : 2 + 2 * iteration]
    at = 2 + 2 * iteration
    state = None
    if iteration > 2:
        state = refs[at][...]
        at += 1
    scaled_ref, weights, downs = refs[at], refs[at + 1 : at + 5], refs[at + 5 : at + 7]
    part_ref, own_x_ref, kept_ref, mix_ref, *rest = refs[at + 7 :]
    squares_ref = rest[-1]
    x_ref, pre_ref = rest[:2]
    tokens, features = part_ref.shape

    @on_core(0)
    def _():
        products(scaled_ref, weights, pre_ref)

    @on_core(1)
    def _():
        pre_ref[...] = ready_ref[...]

    pres = (*pres, pre_ref)
    fresh = own_ref[...] + other_ref[...]
    kept, mix, entries = gram_and_weights(fresh, state, iteration - 1, cells)
    kept_ref[...] = kept
    mix_ref[...] = weight_rows(mix, entries, iteration == 2)
    total = mix[0]
    for i in range(1, iteration):
        total = total + mix[i]
    base = (0.5 * mix[0]) * start_row(first_ref, features)

    def step(h, _):
        at = pl.ds(pl.multiple_of(16 * h, 16), 16)
        rows = total * first_ref[at, :features].astype(F32) + base
        for i in range(1, iteration):
            rows = rows + (0.5 * mix[i]) * outs[i - 1][at, :].astype(F32)
        x_ref[at, :] = rows
        squares_ref[at, :] = squares_of(rows)
        return 0

    lax.fori_loop(0, tokens // 16, step, 0)
    own_x_ref[...] = own_rows(x_ref, order)
    factor = lane_rsqrt(squares_ref, features)

    def mixed(start, size):
        accum = mix[0] * pres[0][start : start + size]
        for i in range(1, iteration):
            accum = accum + mix[i] * pres[i][start : start + size]
        return accum

    send_block(mixed, factor, downs, part_ref)


def folded_lanes(values):
    pieces = [values[:, n : n + 128] for n in range(0, values.shape[1], 128)]
    while len(pieces) > 1:
        pieces = [a + b for a, b in zip(pieces[::2], pieces[1::2])]
    return pieces[0]


def summed(values):
    return jnp.sum(jnp.sum(values, axis=0, keepdims=True), axis=1, keepdims=True)


def gram_row(sums, first):
    row = lane_row([summed(s) for s in sums])
    if first is not None:
        lane = lax.broadcasted_iota(jnp.int32, (1, 128), 1)
        row = row + jnp.where(lane == 8, summed(first), 0.0)
    return jnp.concatenate([row, jnp.zeros((7, 128), F32)], axis=0)


def misfit_body(iteration, first_ref, out_ref, x_ref, gain_ref, *refs):
    befores = refs[:iteration]
    row_ref, scaled_ref, *kept = refs[iteration:]
    tokens, features = x_ref.shape

    def step(h, sums):
        at = pl.ds(pl.multiple_of(16 * h, 16), 16)
        image = first_ref[at, :features].astype(F32) + 0.5 * out_ref[at, :].astype(F32)
        scaled_ref[at, :] = (image * gain_ref[...]).astype(BF16)
        misfit = image - x_ref[at, :]
        if kept:
            kept[0][at, :] = misfit
        pairs = [(misfit, befores[j][at, :]) for j in range(iteration)] + [(misfit, misfit)]
        if iteration == 1:
            pairs.append((befores[0][at, :], befores[0][at, :]))
        prods = [folded_lanes(a * b) for a, b in pairs]
        return tuple(s + p[:8] + p[8:] for s, p in zip(sums, prods))

    count = iteration + 1 + (iteration == 1)
    zero = tuple(jnp.zeros((8, 128), F32) for _ in range(count))
    sums = lax.fori_loop(0, tokens // 16, step, zero)
    row_ref[...] = gram_row(sums[: iteration + 1], sums[-1] if iteration == 1 else None)


def last_misfit_body(inject_ref, *refs):
    outs, xs, row_ref = refs[: ITERS - 1], refs[ITERS - 1 : -1], refs[-1]
    inject = inject_ref[...].astype(F32)
    misfits = [xs[0][...]]
    for out_ref, x_ref in zip(outs, xs):
        misfits.append(inject + 0.5 * out_ref[...].astype(F32) - x_ref[...])
    row = gram_row([folded_lanes(misfits[-1] * m) for m in misfits], None)
    for d in range(0, row_ref.shape[0], 8):
        row_ref[d : d + 8] = row


def final_body(cells, rows_ref, inject_ref, start_ref, state_ref, *refs):
    outs, (x_ref, mix_ref) = refs[: ITERS - 1], refs[ITERS - 1 :]
    fresh = rows_ref[0:8]
    for h in range(8, rows_ref.shape[0], 8):
        fresh = fresh + rows_ref[h : h + 8]
    _, mix, entries = gram_and_weights(fresh, state_ref[...], ITERS - 1, cells)
    mix_ref[...] = weight_rows(mix, entries, False)
    inject = inject_ref[...].astype(F32)
    x = mix[0] * start_ref[...]
    for i in range(1, ITERS):
        x = x + mix[i] * (inject + 0.5 * outs[i - 1][...].astype(F32))
    x_ref[...] = x


def local(inject, w_gate, w_up, w_down, gain):
    rows, features = inject.shape[1:]
    sections = lax.axis_size("section")
    groups = lax.axis_size("dp")
    chips = groups // 2
    tokens = rows * chips
    cells = float(rows * groups * features)
    hidden = w_gate.shape[2]
    order = RING if chips == len(RING) else tuple(range(chips))
    same_core = [[2 * h + c for h in order] for c in range(2)]
    across = [(d, d ^ 1) for d in range(groups)]
    ahead = [(s, (s + 1) % sections) for s in range(sections)]
    ahead_across = [
        (s * groups + d, (s + 1) % sections * groups + (d ^ 1))
        for s in range(sections)
        for d in range(groups)
    ]

    def to_chips(array):
        return lax.all_to_all(array, "dp", 0, 0, tiled=True, axis_index_groups=same_core)

    def to_all(block):
        wider = jnp.broadcast_to(block[None], (chips, *block.shape))
        return to_chips(wider).reshape(chips * block.shape[0], block.shape[1])

    shape = jax.ShapeDtypeStruct
    mine = inject[0]
    mine_w = [w_gate[0].T, w_up[0].T, w_down[0]]
    part0 = pallas(start_body, shape((8, features // 8), BF16), "start", 12)(gain, *mine_w)
    other_w = [lax.ppermute(w, "dp", across) for w in mine_w]
    near = lax.ppermute(part0, "section", ahead)
    far = lax.ppermute(part0, ("section", "dp"), ahead_across)
    start_part = (near.astype(F32) + far.astype(F32)).astype(BF16)
    first = to_all(jnp.concatenate([mine, start_part], axis=1))

    part_shape = shape((tokens, features), BF16)
    wide_shape = shape((tokens, features), F32)
    own_shape = shape((rows, features), F32)
    small = shape((8, 128), F32)
    scaled_shape = shape((tokens, features), BF16)
    pre_shape = shape((4 * hidden, tokens), F32)
    squares = pltpu.VMEM((tokens, 128), F32)
    weights = [mine_w[0], mine_w[1], other_w[0], other_w[1]]
    downs = [mine_w[2], other_w[2]]
    pres = []
    cost = pl.CostEstimate(
        flops=8 * hidden * tokens * features,
        bytes_accessed=8 * hidden * features,
        transcendentals=0,
    )
    misfits, gathered, own_outs, own_xs, mixing = [], [], [], [], []
    state = row = None
    for iteration in range(1, ITERS):
        if iteration == 1:
            body = functools.partial(first_block_body, order)
            shapes = (part_shape, wide_shape, own_shape, pre_shape)
            held = [pltpu.VMEM((tokens, features), BF16), squares]
            part, x, own_x, pre = pallas(body, shapes, "block1", 12, held)(
                first, gain, *weights, *downs
            )
            pres.append(pre)
            misfits.append(x)
        else:
            body = functools.partial(block_body, iteration, cells, order)
            carried = [] if state is None else [state]
            ready = pallas(products_body, pre_shape, f"products{iteration}", 12, cost=cost)(
                scaled, *weights
            )
            row, ready = lax.optimization_barrier((row, ready))
            other_row = lax.ppermute(row, "dp", across)
            shapes = [part_shape, own_shape, small, small]
            held = [squares]
            if iteration < ITERS - 1:
                shapes += [wide_shape, pre_shape]
            else:
                held = [pltpu.VMEM((tokens, features), F32), pltpu.VMEM(pre_shape.shape, F32), squares]
            part, own_x, state, mix, *rest = pallas(body, shapes, f"block{iteration}", 12, held)(
                row, other_row, first, *gathered, ready, *pres, *carried, scaled, *weights, *downs
            )
            x, pre = rest if rest else (None, None)
            pres.append(pre)
            if iteration == 2:
                mixing.append(mix[1, :HIST])
            mixing.append(mix[0, :HIST])
        own_xs.append(own_x)
        total = jnp.sum(to_chips(part.reshape(chips, rows, features)).astype(F32), axis=0)
        before = lax.ppermute((own_xs[-1] + total).astype(BF16), "section", ahead)
        own_outs.append(before)
        if iteration < ITERS - 1:
            gathered.append(to_all(before))
            shapes = [small, scaled_shape] + [wide_shape] * (iteration < ITERS - 2)
            row, scaled, *misfit = pallas(
                functools.partial(misfit_body, iteration), shapes, f"misfit{iteration}", 12
            )(first, gathered[-1], x, gain, *misfits)
            misfits += misfit
    copies = shape((8 * groups, 128), F32)
    sums = pallas(last_misfit_body, copies, "last_misfit", 8)(mine, *own_outs, *own_xs)
    sums = lax.all_to_all(sums, "dp", 0, 0, tiled=True)
    iterate, mix = pallas(functools.partial(final_body, cells), (own_shape, small), "final", 8)(
        sums, mine, own_xs[0], state, *own_outs
    )
    mixing.append(mix[0, :HIST])
    return iterate[None], jnp.stack(mixing)[None]


def solution(mesh):
    placed = (
        P("section", "dp", None),
        P("section", None, "dp"),
        P("section", None, "dp"),
        P("section", "dp", None),
        P("section", None),
    )
    return jax.shard_map(
        local,
        mesh=mesh,
        in_specs=placed,
        out_specs=(P("section", "dp", None), P("section", None, None)),
        check_vma=False,
    )
```
